32 devices in a mesh: pc: 4 (over z), pr: 8 (over y, x, core).
Axes of the slice: x: 2, y: 2, z: 4, core: 2. Of those that a mesh axis runs over, the one named last changes fastest.
Arguments:
- panel_in: float32 [4096, 8, 256], P('pr', 'pc')
- trail_in: float32 [4096, 2048], P('pr', 'pc')
Outputs:
- output 1: float32 [4096, 8, 256], P('pr', 'pc')
- output 2: float32 [4096, 2048], P('pr', 'pc')
All inputs are finite; a program needn't handle non-finite values.
Results may differ from the reference program's by a relative error of at most 0.001.
Values sent between devices are 32-bit elements.
A program may use at most 1 GiB of HBM per device.

```python
import jax
import jax.numpy as jnp
from jax import lax

N = 4096
NB = 256
K = 8
PR = 8
PC = 4
RANK = 2048

BLOCKS = N // NB
ROW_BLOCKS = BLOCKS // PR
TRAIL_COLS = N - K * NB
PREC_HIGH = lax.Precision.HIGHEST


def rows_to_owner(full_mat):
    col_width = full_mat.shape[1]
    return full_mat.reshape(ROW_BLOCKS, PR, NB, col_width).transpose(1, 0, 2, 3).reshape(N, col_width)


def rows_from_owner(stored):
    col_width = stored.shape[1]
    return stored.reshape(PR, ROW_BLOCKS, NB, col_width).transpose(1, 0, 2, 3).reshape(N, col_width)


def cols_to_owner(full_mat):
    block_count = full_mat.shape[1] // NB
    return full_mat.reshape(N, block_count // PC, PC, NB).transpose(0, 2, 1, 3).reshape(N, block_count, NB)


def cols_from_owner(stored):
    block_count = stored.shape[1]
    return stored.reshape(N, PC, block_count // PC, NB).transpose(0, 2, 1, 3).reshape(N, block_count * NB)


def build_layout(full_mat):
    row_major = rows_to_owner(full_mat)
    panel_in = cols_to_owner(row_major[:, :K * NB])
    trail_in = cols_to_owner(row_major[:, K * NB:]).reshape(N, TRAIL_COLS)
    return {"panel_in": panel_in, "trail_in": trail_in}


def setup_inputs(seed: int = 0) -> dict:
    key_low, key_diag = jax.random.split(jax.random.key(seed))
    factor = jax.random.normal(key_low, (N, RANK), jnp.float32)
    diag_shift = 0.5 + jax.random.uniform(key_diag, (N,), jnp.float32)
    low_rank = jnp.dot(factor, factor.T, precision=PREC_HIGH) / RANK
    full_mat = 0.5 * (low_rank + low_rank.T) + jnp.diag(diag_shift)
    return build_layout(full_mat)


def reference(panel_in, trail_in):
    stored = jnp.concatenate([cols_from_owner(panel_in), cols_from_owner(trail_in.reshape(N, BLOCKS - K, NB))], axis=1)
    work_mat = rows_from_owner(stored)
    factor_cols = []
    kept_rows = []
    for panel_step in range(K):
        l_diag = jnp.linalg.cholesky(work_mat[:NB, :NB])
        below_diag = lax.linalg.triangular_solve(l_diag, work_mat[NB:, :NB], left_side=False, lower=True, transpose_a=True)
        factor_cols.append(jnp.concatenate([jnp.zeros((panel_step * NB, NB), work_mat.dtype), l_diag, below_diag], axis=0))
        kept_rows.append(work_mat[:NB, (K - panel_step) * NB:])
        work_mat = work_mat[NB:, NB:] - jnp.dot(below_diag, below_diag.T, precision=PREC_HIGH)
    panel_full = jnp.concatenate(factor_cols, axis=1)
    trail_full = jnp.concatenate(kept_rows + [work_mat], axis=0)
    panel_out = cols_to_owner(rows_to_owner(panel_full))
    trail_out = cols_to_owner(rows_to_owner(trail_full)).reshape(N, TRAIL_COLS)
    return panel_out, trail_out
```

```python
import functools

import jax
import jax.numpy as jnp
from jax import lax
from jax.experimental import pallas as pl
from jax.experimental.pallas import tpu as pltpu
from jax.sharding import PartitionSpec as P

HI = lax.Precision.HIGHEST
NB = 256
B = 32
T = B // 8


def bc(v, s):
    return jnp.broadcast_to(v[s:s+1, :], (8, 128))

def factor(z, lout, wout):
    sub = lax.broadcasted_iota(jnp.int32, (8,128), 0)
    lane = lax.broadcasted_iota(jnp.int32, (8,128), 1)
    for b in range(NB//B):
        r0 = b*B; v0 = r0//128; d0 = r0-128*v0
        xa = [[z[r0+8*t:r0+8*t+8, 128*v:128*v+128] for v in range(v0,2)] for t in range(T)]
        cols = [[None]*T for _ in range(B)]
        for j in range(B):
            for t in range(j//8, T):
                cols[j][t] = jnp.broadcast_to(xa[t][0][:, d0+j:d0+j+1], (8,128))
        xs = []
        for t in range(T):
            row = list(xa[t])
            for v in range(v0):
                row.append(z[r0+8*t:r0+8*t+8, 128*v:128*v+128])
            e = jnp.where(lane < d0, xa[t][0], jnp.where(lane - d0 == sub + 8*t, 1.0, 0.0))
            row.append(e)
            xs.append(row)
        nv = len(xs[0])
        sv = [jnp.zeros((8,128), jnp.float32) for _ in range(T)]
        piv = bc(cols[0][0], 0)
        for p in range(B):
            tp, sp = divmod(p, 8)
            s = lax.rsqrt(piv)
            m = None
            if p < B-1:
                t1, s1 = divmod(p+1, 8)
                m = bc(cols[p][t1], s1)*s
                piv = bc(cols[p+1][t1], s1) - m*m
            l = [None]*T
            for t in range(tp, T):
                l[t] = cols[p][t]*s
            for j in range(p+1, B):
                mj = m if j == p+1 else bc(l[j//8], j%8)
                for t in range(j//8, T):
                    cols[j][t] = cols[j][t] - l[t]*mj
            lm = jnp.where(sub > sp, l[tp], 0.0)
            sv[tp] = jnp.where(sub == sp, s, sv[tp])
            for v in range(nv):
                u = bc(xs[tp][v], sp)*s
                if sp < 7:
                    xs[tp][v] = xs[tp][v] - lm*u
                for t in range(tp+1, T):
                    xs[t][v] = xs[t][v] - l[t]*u
        for t in range(T):
            for v in range(nv):
                xs[t][v] = xs[t][v]*sv[t]
        na = 2 - v0
        urow, rrow, wrow = [], [], []
        for t in range(T):
            a = list(xs[t][:na]); e = list(xs[t][na:])
            a0 = jnp.where(lane - d0 >= sub + 8*t, a[0], 0.0)
            ua = [jnp.zeros((8,128), jnp.float32)]*v0 + [a0] + a[1:]
            e[v0] = jnp.where(lane < d0 + B, e[v0], 0.0)
            wr = e + [jnp.zeros((8,128), jnp.float32)]*(1-v0)
            mid = jnp.where(lane < d0 + B, e[v0], a[0])
            rr = e[:v0] + [mid] + a[1:]
            urow.append(jnp.concatenate(ua, axis=1)); wrow.append(jnp.concatenate(wr, axis=1)); rrow.append(jnp.concatenate(rr, axis=1))
        U = jnp.concatenate(urow, axis=0); W = jnp.concatenate(wrow, axis=0); R = jnp.concatenate(rrow, axis=0)
        wout[r0:r0+B, :] = W
        LT = U.T
        lout[:, r0:r0+B] = LT
        lane2 = lax.broadcasted_iota(jnp.int32, (1, NB), 1)
        inb = (lane2 >= r0) & (lane2 < r0+B)
        def upd(lo, hi):
            if lo >= hi: return
            old = z[lo:hi, :]
            old = jnp.where(inb, 0.0, old)
            z[lo:hi, :] = old - lax.dot_general(LT[lo:hi], R, (((1,),(0,)),((),())), precision=HI, preferred_element_type=jnp.float32)
        upd(r0+B, min(r0+2*B, NB))
        upd(r0+2*B, NB)

def dot_nt(a, b):
    return lax.dot_general(a, b, (((1,), (1,)), ((), ())), precision=HI, preferred_element_type=jnp.float32)


def dot_nn(a, b):
    return lax.dot_general(a, b, (((1,), (0,)), ((), ())), precision=HI, preferred_element_type=jnp.float32)


def rows_at(block, count):
    return pl.ds(pl.multiple_of(block * NB, NB), count * NB)


def over_rows(first, stop, fn):
    total = stop - first
    pairs = total // 2

    def step(i, _):
        fn(first + 2 * i, 2)
        return 0

    lax.fori_loop(0, pairs, step, 0)

    @pl.when(total % 2 == 1)
    def _():
        fn(stop - 1, 1)


def local_kernel(g0, g1, low, up, trail, panel_out, trail_out, col, tt, ss, z, lo, wo, sem_a, sem_r, sem_t, sem_s):
    my_row = lax.axis_index("pr")
    my_col = lax.axis_index("pc")
    K = 8

    def copy_a(k):
        g = g0 if k < 4 else g1
        return pltpu.make_async_copy(g.at[k % 4, pl.ds(k * NB, (K - k) * NB), :], col.at[k, pl.ds(k * NB, (K - k) * NB), :], sem_a.at[k])

    def copy_r(k):
        return pltpu.make_async_copy(low.at[k % 4, k // 4], col.at[k, pl.ds(K * NB, NB), :], sem_r.at[k])

    def copy_t(k):
        return pltpu.make_async_copy(up.at[k], tt.at[k], sem_t.at[k])

    copy_s = pltpu.make_async_copy(trail, ss, sem_s)
    for k in range(K):
        copy_a(k).start()
        copy_r(k).start()
        copy_t(k).start()
    copy_s.start()
    for k in range(K):
        copy_a(k).wait()
        copy_r(k).wait()
        copy_t(k).wait()
    copy_s.wait()

    def step(k, _):
        def left(m, _):
            rhs = col[m, rows_at(k, 1), :]

            def upd(block, count):
                sl = rows_at(block, count)
                col[k, sl, :] = col[k, sl, :] - dot_nt(col[m, sl, :], rhs)

            over_rows(k, K + 1, upd)
            tt[k] = tt[k] - dot_nn(rhs, tt[m])
            return 0

        lax.fori_loop(0, k, left, 0)

        @pl.when(k == my_row)
        def _():
            trail_out[0:NB, :] = tt[k]

        z[...] = col[k, rows_at(k, 1), :]
        factor(z, lo, wo)
        col[k, rows_at(k, 1), :] = lo[...]

        def solve(block, count):
            sl = rows_at(block, count)
            col[k, sl, :] = dot_nt(col[k, sl, :], wo[...])

        over_rows(k + 1, K + 1, solve)
        tt[k] = dot_nn(wo[...], tt[k])
        ss[...] = ss[...] - dot_nn(col[k, K * NB:(K + 1) * NB, :], tt[k])

        @pl.when(my_col == k % 4)
        def _():
            slot = k // 4
            panel_out[slot, NB:, :] = col[k, K * NB:(K + 1) * NB, :]

            @pl.when(my_row >= k)
            def _():
                panel_out[slot, 0:NB, :] = col[k, rows_at(my_row, 1), :]

            @pl.when(my_row < k)
            def _():
                panel_out[slot, 0:NB, :] = jnp.zeros((NB, NB), jnp.float32)
        return 0

    lax.fori_loop(0, K, step, 0)
    trail_out[NB:, :] = ss[...]


def solution(mesh):
    vmem = pl.BlockSpec(memory_space=pltpu.VMEM)
    hbm = pl.BlockSpec(memory_space=pl.ANY)
    f32 = jnp.float32
    call = pl.pallas_call(
        local_kernel,
        out_shape=[jax.ShapeDtypeStruct((2, 512, NB), f32), jax.ShapeDtypeStruct((512, 512), f32)],
        in_specs=[hbm] * 5,
        out_specs=[vmem, vmem],
        scratch_shapes=[
            pltpu.VMEM((8, 9 * NB, NB), f32),
            pltpu.VMEM((8, NB, 512), f32),
            pltpu.VMEM((NB, 512), f32),
            pltpu.VMEM((NB, NB), f32),
            pltpu.VMEM((NB, NB), f32),
            pltpu.VMEM((NB, NB), f32),
            pltpu.SemaphoreType.DMA((8,)),
            pltpu.SemaphoreType.DMA((8,)),
            pltpu.SemaphoreType.DMA((8,)),
            pltpu.SemaphoreType.DMA,
        ],
        compiler_params=pltpu.CompilerParams(vmem_limit_bytes=60 * 1024 * 1024),
    )

    def local_part(panel_tile, trail_tile):
        slots = panel_tile.transpose(1, 0, 2)
        g0 = lax.all_gather(slots[0, :NB], ("pc", "pr"), axis=0, tiled=False).reshape(4, 8 * NB, NB)
        g1 = lax.all_gather(slots[1, :NB], ("pc", "pr"), axis=0, tiled=False).reshape(4, 8 * NB, NB)
        low = lax.all_gather(slots[:, NB:], "pc", axis=0, tiled=False)
        up = lax.all_gather(trail_tile[:NB], "pr", axis=0, tiled=False)
        p, t = call(g0, g1, low, up, trail_tile[NB:])
        return p.transpose(1, 0, 2), t

    sp, st = P("pr", "pc", None), P("pr", "pc")
    return jax.shard_map(local_part, mesh=mesh, in_specs=(sp, st), out_specs=(sp, st), check_vma=False)
```

```python
import functools

import jax
import jax.numpy as jnp
from jax import lax
from jax.experimental import pallas as pl
from jax.experimental.pallas import tpu as pltpu
from jax.sharding import PartitionSpec as P

HI = lax.Precision.HIGHEST
NB = 256
B = 32
T = B // 8


def bc(v, s):
    return jnp.broadcast_to(v[s:s+1, :], (8, 128))

def factor(z, lout, wout, hook):
    sub = lax.broadcasted_iota(jnp.int32, (8,128), 0)
    lane = lax.broadcasted_iota(jnp.int32, (8,128), 1)
    for b in range(NB//B):
        r0 = b*B; v0 = r0//128; d0 = r0-128*v0
        hook(b)
        xa = [[z[r0+8*t:r0+8*t+8, 128*v:128*v+128] for v in range(v0,2)] for t in range(T)]
        cols = [[None]*T for _ in range(B)]
        for j in range(B):
            for t in range(j//8, T):
                cols[j][t] = jnp.broadcast_to(xa[t][0][:, d0+j:d0+j+1], (8,128))
        xs = []
        for t in range(T):
            row = list(xa[t])
            for v in range(v0):
                row.append(z[r0+8*t:r0+8*t+8, 128*v:128*v+128])
            e = jnp.where(lane < d0, xa[t][0], jnp.where(lane - d0 == sub + 8*t, 1.0, 0.0))
            row.append(e)
            xs.append(row)
        nv = len(xs[0])
        sv = [jnp.zeros((8,128), jnp.float32) for _ in range(T)]
        piv = bc(cols[0][0], 0)
        for p in range(B):
            tp, sp = divmod(p, 8)
            s = lax.rsqrt(piv)
            m = None
            if p < B-1:
                t1, s1 = divmod(p+1, 8)
                m = bc(cols[p][t1], s1)*s
                piv = bc(cols[p+1][t1], s1) - m*m
            l = [None]*T
            for t in range(tp, T):
                l[t] = cols[p][t]*s
            for j in range(p+1, B):
                mj = m if j == p+1 else bc(l[j//8], j%8)
                for t in range(j//8, T):
                    cols[j][t] = cols[j][t] - l[t]*mj
            lm = jnp.where(sub > sp, l[tp], 0.0)
            sv[tp] = jnp.where(sub == sp, s, sv[tp])
            for v in range(nv):
                u = bc(xs[tp][v], sp)*s
                if sp < 7:
                    xs[tp][v] = xs[tp][v] - lm*u
                for t in range(tp+1, T):
                    xs[t][v] = xs[t][v] - l[t]*u
        for t in range(T):
            for v in range(nv):
                xs[t][v] = xs[t][v]*sv[t]
        na = 2 - v0
        urow, rrow, wrow = [], [], []
        for t in range(T):
            a = list(xs[t][:na]); e = list(xs[t][na:])
            a0 = jnp.where(lane - d0 >= sub + 8*t, a[0], 0.0)
            ua = [jnp.zeros((8,128), jnp.float32)]*v0 + [a0] + a[1:]
            e[v0] = jnp.where(lane < d0 + B, e[v0], 0.0)
            wr = e + [jnp.zeros((8,128), jnp.float32)]*(1-v0)
            mid = jnp.where(lane < d0 + B, e[v0], a[0])
            rr = e[:v0] + [mid] + a[1:]
            urow.append(jnp.concatenate(ua, axis=1)); wrow.append(jnp.concatenate(wr, axis=1)); rrow.append(jnp.concatenate(rr, axis=1))
        U = jnp.concatenate(urow, axis=0); W = jnp.concatenate(wrow, axis=0); R = jnp.concatenate(rrow, axis=0)
        wout[r0:r0+B, :] = W
        LT = U.T
        lout[:, r0:r0+B] = LT
        lane2 = lax.broadcasted_iota(jnp.int32, (1, NB), 1)
        inb = (lane2 >= r0) & (lane2 < r0+B)
        def upd(lo, hi):
            if lo >= hi: return
            old = z[lo:hi, :]
            old = jnp.where(inb, 0.0, old)
            z[lo:hi, :] = old - lax.dot_general(LT[lo:hi], R, (((1,),(0,)),((),())), precision=HI, preferred_element_type=jnp.float32)
        upd(r0+B, min(r0+2*B, NB))
        upd(r0+2*B, NB)

MESH = pl.DeviceIdType.MESH
K = 8


def dot_nt(a, b):
    return lax.dot_general(a, b, (((1,), (1,)), ((), ())), precision=HI, preferred_element_type=jnp.float32)


def dot_nn(a, b):
    return lax.dot_general(a, b, (((1,), (0,)), ((), ())), precision=HI, preferred_element_type=jnp.float32)


def rows_at(block, count=1):
    return pl.ds(pl.multiple_of(block * NB, NB), count * NB)


def over_rows(first, stop, fn):
    total = stop - first

    def step(i, _):
        fn(first + 2 * i, 2)
        return 0

    lax.fori_loop(0, total // 2, step, 0)

    @pl.when(total % 2 == 1)
    def _():
        fn(stop - 1, 1)


def chip_kernel(panel, trail, panel_out, trail_out, col, wb, rw, tt, ss, rst, z, lo,
                rec_a, rec_w, rec_t, rec_r, rec_s, rec_o, snd_z, snd_p, snd_l, snd_w, snd_t, snd_r, snd_s, snd_o):
    c = lax.axis_index("pc")
    r = lax.axis_index("pr")
    core = r % 2
    p = r // 2
    px = 2 * (p // 2) + (1 - p % 2)
    py = 2 * (1 - p // 2) + p % 2
    pd = 3 - p
    is0 = core == 0
    is1 = core == 1

    def remote(src, dst, send, recv, c2, r2):
        return pltpu.make_async_remote_copy(src_ref=src, dst_ref=dst, send_sem=send, recv_sem=recv, device_id=(c2, r2), device_id_type=MESH)

    def z_copy(s, i):
        k = c + 4 * s
        return remote(panel.at[s, 0:NB, :], col.at[k, rows_at(r), :], snd_z.at[s, i], rec_a.at[k, r], (c + i) % 4, 2 * p)

    def z_home(s):
        k = c + 4 * s
        return pltpu.make_async_copy(panel.at[s, 0:NB, :], col.at[k, rows_at(r), :], rec_a.at[k, r])

    def z_send(s):
        k = c + 4 * s

        @pl.when((r >= k) & is0)
        def _():
            z_home(s).start()

        @pl.when((r >= k) & is1)
        def _():
            z_copy(s, 0).start()

        @pl.when(r >= k)
        def _():
            for i in (1, 3, 2):
                z_copy(s, i).start()

    def z_done(s):
        k = c + 4 * s

        @pl.when((r >= k) & is1)
        def _():
            z_copy(s, 0).wait_send()

        @pl.when(r >= k)
        def _():
            for i in (1, 2, 3):
                z_copy(s, i).wait_send()

    def t_copy(i):
        q = (p + i) % 4
        return remote(trail.at[0:NB, :], tt.at[r], snd_t.at[i], rec_t.at[r], c, 2 * q + 1)

    def r_copy(s, i):
        k = c + 4 * s
        return remote(panel.at[s, NB:2 * NB, :], rw.at[k, rows_at(core), :], snd_r.at[s, i], rec_r.at[k, core], (c + i) % 4, 2 * p + 1)

    def s_copy():
        return remote(trail.at[NB:2 * NB, :], ss.at[rows_at(core), :], snd_s, rec_s.at[core], c, r + 1)

    def other_sends():
        for i in (1, 2, 3):
            t_copy(i).start()
        for s in (0, 1):
            for i in (1, 3, 2):
                r_copy(s, i).start()

        @pl.when(is0)
        def _():
            t_copy(0).start()
            r_copy(0, 0).start()
            r_copy(1, 0).start()
            s_copy().start()

        @pl.when(is1)
        def _():
            pltpu.make_async_copy(trail.at[0:NB, :], tt.at[r], rec_t.at[r]).start()
            for s in (0, 1):
                pltpu.make_async_copy(panel.at[s, NB:2 * NB, :], rw.at[c + 4 * s, rows_at(core), :], rec_r.at[c + 4 * s, core]).start()
            pltpu.make_async_copy(trail.at[NB:2 * NB, :], ss.at[rows_at(core), :], rec_s.at[core]).start()

    def other_done():
        for i in (1, 2, 3):
            t_copy(i).wait_send()
            for s in (0, 1):
                r_copy(s, i).wait_send()

        @pl.when(is0)
        def _():
            t_copy(0).wait_send()
            r_copy(0, 0).wait_send()
            r_copy(1, 0).wait_send()
            s_copy().wait_send()

    def blk(k, j):
        return col.at[k, rows_at(j), :]

    def got_a(k, j):
        pltpu.make_async_copy(blk(k, j), blk(k, j), rec_a.at[k, j]).wait()

    def p_copy(k, j, n, q):
        return remote(blk(k, j), blk(k, j), snd_p.at[k, n], rec_a.at[k, j], c, 2 * q)

    own_sends = ((2 * p, 0, px), (2 * p, 1, py), (2 * p + 1, 2, py), (2 * p + 1, 3, px))
    fwd_sends = ((2 * px, 4, py), (2 * py + 1, 5, px))
    last_rows = (2 * px + 1, 2 * py, 2 * pd, 2 * pd + 1)

    def stage(k, lowest, sends, rows):
        for j in rows:
            @pl.when(j >= lowest)
            def _(j=j):
                got_a(k, j)
        for j, n, q in sends:
            @pl.when(j >= lowest)
            def _(j=j, n=n, q=q):
                p_copy(k, j, n, q).start()

    def stage1(k, lowest):
        stage(k, lowest, own_sends, (2 * p, 2 * p + 1))

    def stage2(k, lowest):
        stage(k, lowest, fwd_sends, (2 * px, 2 * py + 1))

    def stage3(k, lowest):
        stage(k, lowest, (), last_rows)
        for j, n, q in own_sends + fwd_sends:
            @pl.when(j >= lowest)
            def _(j=j, n=n, q=q):
                p_copy(k, j, n, q).wait_send()

    def l_copy(k, j):
        return remote(blk(k, j), blk(k, j), snd_l.at[k, j], rec_a.at[k, j], c, r + 1)

    def w_copy(k):
        return remote(wb.at[k], wb.at[k], snd_w.at[k], rec_w.at[k], c, r + 1)

    def each_row(first, fn):
        lax.fori_loop(first, K, lambda j, _: (fn(j), 0)[1], 0)

    def o_top():
        return remote(rst, trail_out.at[0:NB, :], snd_o.at[0], rec_o.at[0], c, r - 1)

    def o_low():
        return remote(ss.at[0:NB, :], trail_out.at[NB:2 * NB, :], snd_o.at[1], rec_o.at[1], c, r - 1)

    def o_row(s):
        return remote(rw.at[c + 4 * s, 0:NB, :], panel_out.at[s, NB:2 * NB, :], snd_o.at[2 + s], rec_o.at[2 + s], c, r - 1)

    z_send(0)

    @pl.when(is0)
    def _():
        @pl.when(p == 0)
        def _():
            got_a(0, 0)
            p_copy(0, 0, 0, px).start()
            p_copy(0, 0, 1, py).start()

        @pl.when(p != 0)
        def _():
            got_a(0, 0)

        @pl.when(p == 1)
        def _():
            p_copy(0, 0, 4, py).start()

        z_send(1)
        other_sends()

        def step(k, _):
            @pl.when(k > 0)
            def _():
                stage3(k, k)
                each_row(k - 1, lambda j: l_copy(k - 1, j).start())

            def left(m, _):
                rhs = col[m, rows_at(k), :]

                def upd(block, count):
                    sl = rows_at(block, count)
                    col[k, sl, :] = col[k, sl, :] - dot_nt(col[m, sl, :], rhs)

                over_rows(k, K, upd)
                return 0

            lax.fori_loop(0, k, left, 0)
            z[...] = col[k, rows_at(k), :]

            def hook(b):
                if b == 1:
                    @pl.when(k == 0)
                    def _():
                        stage1(0, 1)
                if b == 2:
                    @pl.when(k < K - 1)
                    def _():
                        stage1(k + 1, k + 1)
                if b == 5:
                    @pl.when(k == 0)
                    def _():
                        stage2(0, 1)
                if b == 7:
                    @pl.when(k < K - 1)
                    def _():
                        stage2(k + 1, k + 1)

            factor(z, lo, wb.at[k], hook)

            @pl.when(k == 0)
            def _():
                stage3(0, 1)

                @pl.when(p == 0)
                def _():
                    p_copy(0, 0, 0, px).wait_send()
                    p_copy(0, 0, 1, py).wait_send()

                @pl.when(p == 1)
                def _():
                    p_copy(0, 0, 4, py).wait_send()

            col[k, rows_at(k), :] = lo[...]
            w_copy(k).start()

            def solve(block, count):
                sl = rows_at(block, count)
                col[k, sl, :] = dot_nt(col[k, sl, :], wb[k])

            over_rows(k + 1, K, solve)
            return 0

        lax.fori_loop(0, K, step, 0)
        l_copy(K - 1, K - 1).start()

    @pl.when(is1)
    def _():
        z_send(1)
        other_sends()
        for i in (0, 1):
            pltpu.make_async_copy(ss.at[rows_at(i), :], ss.at[rows_at(i), :], rec_s.at[i]).wait()

        def step(k, _):
            pltpu.make_async_copy(tt.at[k], tt.at[k], rec_t.at[k]).wait()
            for i in (0, 1):
                pltpu.make_async_copy(rw.at[k, rows_at(i), :], rw.at[k, rows_at(i), :], rec_r.at[k, i]).wait()

            def left(m, _):
                got_a(m, k)
                lkm = col[m, rows_at(k), :]
                tt[k] = tt[k] - dot_nn(lkm, tt[m])
                rw[k] = rw[k] - dot_nt(rw[m], lkm)
                return 0

            lax.fori_loop(0, k, left, 0)

            @pl.when(k == r)
            def _():
                trail_out[0:NB, :] = tt[k]

            @pl.when(k == r - 1)
            def _():
                rst[...] = tt[k]

            pltpu.make_async_copy(wb.at[k], wb.at[k], rec_w.at[k]).wait()
            tt[k] = dot_nn(wb[k], tt[k])
            rw[k] = dot_nt(rw[k], wb[k])
            ss[...] = ss[...] - dot_nn(rw[k], tt[k])
            return 0

        lax.fori_loop(0, K, step, 0)
        o_low().start()
        o_row(0).start()
        o_row(1).start()
        o_top().start()
        trail_out[NB:2 * NB, :] = ss[NB:2 * NB, :]
        for s in (0, 1):
            panel_out[s, NB:2 * NB, :] = rw[c + 4 * s, NB:2 * NB, :]

        def diag_arrived(k, _):
            got_a(k, k)
            return 0

        lax.fori_loop(0, K, diag_arrived, 0)

    for s in (0, 1):
        k = c + 4 * s

        @pl.when(r >= k)
        def _(s=s, k=k):
            panel_out[s, 0:NB, :] = col[k, rows_at(r), :]

        @pl.when(r < k)
        def _(s=s):
            panel_out[s, 0:NB, :] = jnp.zeros((NB, NB), jnp.float32)

    z_done(0)
    z_done(1)
    other_done()

    @pl.when(is0)
    def _():
        def sent(k, _):
            w_copy(k).wait_send()
            each_row(k, lambda j: l_copy(k, j).wait_send())
            return 0

        lax.fori_loop(0, K, sent, 0)
        for ref, i in ((trail_out.at[0:NB, :], 0), (trail_out.at[NB:2 * NB, :], 1), (panel_out.at[0, NB:2 * NB, :], 2), (panel_out.at[1, NB:2 * NB, :], 3)):
            pltpu.make_async_copy(ref, ref, rec_o.at[i]).wait()

    @pl.when(is1)
    def _():
        o_low().wait_send()
        o_row(0).wait_send()
        o_row(1).wait_send()
        o_top().wait_send()


def solution(mesh):
    vmem = pl.BlockSpec(memory_space=pltpu.VMEM)
    f32 = jnp.float32
    dma = pltpu.SemaphoreType.DMA
    call = pl.pallas_call(
        chip_kernel,
        out_shape=[jax.ShapeDtypeStruct((2, 512, NB), f32), jax.ShapeDtypeStruct((512, 512), f32)],
        in_specs=[vmem, vmem],
        out_specs=[vmem, vmem],
        scratch_shapes=[
            pltpu.VMEM((K, K * NB, NB), f32),
            pltpu.VMEM((K, NB, NB), f32),
            pltpu.VMEM((K, 2 * NB, NB), f32),
            pltpu.VMEM((K, NB, 512), f32),
            pltpu.VMEM((512, 512), f32),
            pltpu.VMEM((NB, 512), f32),
            pltpu.VMEM((NB, NB), f32),
            pltpu.VMEM((NB, NB), f32),
            dma((K, K)), dma((K,)), dma((K,)), dma((K, 2)), dma((2,)), dma((4,)),
            dma((2, 4)), dma((K, 6)), dma((K, K)), dma((K,)), dma((4,)), dma((2, 4)), dma, dma((4,)),
        ],
        compiler_params=pltpu.CompilerParams(vmem_limit_bytes=60 * 1024 * 1024, has_side_effects=True),
    )

    def local_part(panel_tile, trail_tile):
        p, t = call(panel_tile.transpose(1, 0, 2), trail_tile)
        return p.transpose(1, 0, 2), t

    sp, st = P("pr", "pc", None), P("pr", "pc")
    return jax.shard_map(local_part, mesh=mesh, in_specs=(sp, st), out_specs=(sp, st), check_vma=False)
```

```python
import functools

import jax
import jax.numpy as jnp
from jax import lax
from jax.experimental import pallas as pl
from jax.experimental.pallas import tpu as pltpu
from jax.sharding import PartitionSpec as P

HI = lax.Precision.HIGHEST
NB = 256
B = 32
T = B // 8


def bc(v, s):
    return jnp.broadcast_to(v[s:s+1, :], (8, 128))

def factor(z, lout, wout, hook):
    sub = lax.broadcasted_iota(jnp.int32, (8,128), 0)
    lane = lax.broadcasted_iota(jnp.int32, (8,128), 1)
    for b in range(NB//B):
        r0 = b*B; v0 = r0//128; d0 = r0-128*v0
        hook(b)
        xa = [[z[r0+8*t:r0+8*t+8, 128*v:128*v+128] for v in range(v0,2)] for t in range(T)]
        cols = [[None]*T for _ in range(B)]
        for j in range(B):
            for t in range(j//8, T):
                cols[j][t] = jnp.broadcast_to(xa[t][0][:, d0+j:d0+j+1], (8,128))
        xs = []
        for t in range(T):
            row = list(xa[t])
            for v in range(v0):
                row.append(z[r0+8*t:r0+8*t+8, 128*v:128*v+128])
            e = jnp.where(lane < d0, xa[t][0], jnp.where(lane - d0 == sub + 8*t, 1.0, 0.0))
            row.append(e)
            xs.append(row)
        nv = len(xs[0])
        sv = [jnp.zeros((8,128), jnp.float32) for _ in range(T)]
        piv = bc(cols[0][0], 0)
        for p in range(B):
            tp, sp = divmod(p, 8)
            s = lax.rsqrt(piv)
            m = None
            if p < B-1:
                t1, s1 = divmod(p+1, 8)
                m = bc(cols[p][t1], s1)*s
                piv = bc(cols[p+1][t1], s1) - m*m
            l = [None]*T
            for t in range(tp, T):
                l[t] = cols[p][t]*s
            for j in range(p+1, B):
                mj = m if j == p+1 else bc(l[j//8], j%8)
                for t in range(j//8, T):
                    cols[j][t] = cols[j][t] - l[t]*mj
            lm = jnp.where(sub > sp, l[tp], 0.0)
            sv[tp] = jnp.where(sub == sp, s, sv[tp])
            for v in range(nv):
                u = bc(xs[tp][v], sp)*s
                if sp < 7:
                    xs[tp][v] = xs[tp][v] - lm*u
                for t in range(tp+1, T):
                    xs[t][v] = xs[t][v] - l[t]*u
        for t in range(T):
            for v in range(nv):
                xs[t][v] = xs[t][v]*sv[t]
        na = 2 - v0
        urow, rrow, wrow = [], [], []
        for t in range(T):
            a = list(xs[t][:na]); e = list(xs[t][na:])
            a0 = jnp.where(lane - d0 >= sub + 8*t, a[0], 0.0)
            ua = [jnp.zeros((8,128), jnp.float32)]*v0 + [a0] + a[1:]
            e[v0] = jnp.where(lane < d0 + B, e[v0], 0.0)
            wr = e + [jnp.zeros((8,128), jnp.float32)]*(1-v0)
            mid = jnp.where(lane < d0 + B, e[v0], a[0])
            rr = e[:v0] + [mid] + a[1:]
            urow.append(jnp.concatenate(ua, axis=1)); wrow.append(jnp.concatenate(wr, axis=1)); rrow.append(jnp.concatenate(rr, axis=1))
        U = jnp.concatenate(urow, axis=0); W = jnp.concatenate(wrow, axis=0); R = jnp.concatenate(rrow, axis=0)
        wout[r0:r0+B, :] = W
        LT = U.T
        lout[:, r0:r0+B] = LT
        lane2 = lax.broadcasted_iota(jnp.int32, (1, NB), 1)
        inb = (lane2 >= r0) & (lane2 < r0+B)
        def upd(lo, hi):
            if lo >= hi: return
            old = z[lo:hi, :]
            old = jnp.where(inb, 0.0, old)
            z[lo:hi, :] = old - lax.dot_general(LT[lo:hi], R, (((1,),(0,)),((),())), precision=HI, preferred_element_type=jnp.float32)
        upd(r0+B, min(r0+2*B, NB))
        upd(r0+2*B, NB)

MESH = pl.DeviceIdType.MESH
K = 8


def dot_nt(a, b):
    return lax.dot_general(a, b, (((1,), (1,)), ((), ())), precision=HI, preferred_element_type=jnp.float32)


def dot_nn(a, b):
    return lax.dot_general(a, b, (((1,), (0,)), ((), ())), precision=HI, preferred_element_type=jnp.float32)


def rows_at(block, count=1):
    return pl.ds(pl.multiple_of(block * NB, NB), count * NB)


def over_rows(first, stop, fn):
    total = stop - first

    def step(i, _):
        fn(first + 2 * i, 2)
        return 0

    lax.fori_loop(0, total // 2, step, 0)

    @pl.when(total % 2 == 1)
    def _():
        fn(stop - 1, 1)


def chip_kernel(panel, trail, panel_out, trail_out, col, wb, rw, tt, ss, rst, z, lo,
                rec_a, rec_w, rec_t, rec_r, rec_s, rec_o, snd_z, snd_p, snd_l, snd_w, snd_t, snd_r, snd_s, snd_o):
    c = lax.axis_index("pc")
    r = lax.axis_index("pr")
    core = r % 2
    p = r // 2
    px = 2 * (p // 2) + (1 - p % 2)
    py = 2 * (1 - p // 2) + p % 2
    pd = 3 - p
    is0 = core == 0
    is1 = core == 1

    def remote(src, dst, send, recv, c2, r2):
        return pltpu.make_async_remote_copy(src_ref=src, dst_ref=dst, send_sem=send, recv_sem=recv, device_id=(c2, r2), device_id_type=MESH)

    def z_copy(s, i):
        k = c + 4 * s
        return remote(panel.at[s, 0:NB, :], col.at[k, rows_at(r), :], snd_z.at[s, i], rec_a.at[k, r], (c + i) % 4, 2 * p)

    def z_home(s):
        k = c + 4 * s
        return pltpu.make_async_copy(panel.at[s, 0:NB, :], col.at[k, rows_at(r), :], rec_a.at[k, r])

    def z_send(s):
        k = c + 4 * s

        @pl.when((r >= k) & is0)
        def _():
            z_home(s).start()

        @pl.when((r >= k) & is1)
        def _():
            z_copy(s, 0).start()

        @pl.when(r >= k)
        def _():
            for i in (1, 3, 2):
                z_copy(s, i).start()

    def z_done(s):
        k = c + 4 * s

        @pl.when((r >= k) & is1)
        def _():
            z_copy(s, 0).wait_send()

        @pl.when(r >= k)
        def _():
            for i in (1, 2, 3):
                z_copy(s, i).wait_send()

    def t_copy(i):
        q = (p + i) % 4
        return remote(trail.at[0:NB, :], tt.at[r], snd_t.at[i], rec_t.at[r], c, 2 * q + 1)

    def r_copy(s, i):
        k = c + 4 * s
        return remote(panel.at[s, NB:2 * NB, :], rw.at[k, rows_at(core), :], snd_r.at[s, i], rec_r.at[k, core], (c + i) % 4, 2 * p + 1)

    def s_copy():
        return remote(trail.at[NB:2 * NB, :], ss.at[rows_at(core), :], snd_s, rec_s.at[core], c, r + 1)

    def other_sends():
        for i in (1, 2, 3):
            t_copy(i).start()
        for s in (0, 1):
            for i in (1, 3, 2):
                r_copy(s, i).start()

        @pl.when(is0)
        def _():
            t_copy(0).start()
            r_copy(0, 0).start()
            r_copy(1, 0).start()
            s_copy().start()

        @pl.when(is1)
        def _():
            pltpu.make_async_copy(trail.at[0:NB, :], tt.at[r], rec_t.at[r]).start()
            for s in (0, 1):
                pltpu.make_async_copy(panel.at[s, NB:2 * NB, :], rw.at[c + 4 * s, rows_at(core), :], rec_r.at[c + 4 * s, core]).start()
            pltpu.make_async_copy(trail.at[NB:2 * NB, :], ss.at[rows_at(core), :], rec_s.at[core]).start()

    def other_done():
        for i in (1, 2, 3):
            t_copy(i).wait_send()
            for s in (0, 1):
                r_copy(s, i).wait_send()

        @pl.when(is0)
        def _():
            t_copy(0).wait_send()
            r_copy(0, 0).wait_send()
            r_copy(1, 0).wait_send()
            s_copy().wait_send()

    def blk(k, j):
        return col.at[k, rows_at(j), :]

    def got_a(k, j):
        pltpu.make_async_copy(blk(k, j), blk(k, j), rec_a.at[k, j]).wait()

    def p_copy(k, j, n, q):
        return remote(blk(k, j), blk(k, j), snd_p.at[k, n], rec_a.at[k, j], c, 2 * q)

    own_sends = ((2 * p, 0, px), (2 * p, 1, py), (2 * p + 1, 2, py), (2 * p + 1, 3, px))
    fwd_sends = ((2 * px, 4, py), (2 * py + 1, 5, px))
    last_rows = (2 * px + 1, 2 * py, 2 * pd, 2 * pd + 1)

    def stage(k, lowest, sends, rows):
        for j in rows:
            @pl.when(j >= lowest)
            def _(j=j):
                got_a(k, j)
        for j, n, q in sends:
            @pl.when(j >= lowest)
            def _(j=j, n=n, q=q):
                p_copy(k, j, n, q).start()

    def stage1(k, lowest):
        stage(k, lowest, own_sends, (2 * p, 2 * p + 1))

    def stage2(k, lowest):
        stage(k, lowest, fwd_sends, (2 * px, 2 * py + 1))

    def stage3(k, lowest):
        stage(k, lowest, (), last_rows)
        for j, n, q in own_sends + fwd_sends:
            @pl.when(j >= lowest)
            def _(j=j, n=n, q=q):
                p_copy(k, j, n, q).wait_send()

    def l_copy(k, j):
        return remote(blk(k, j), blk(k, j), snd_l.at[k, j], rec_a.at[k, j], c, r + 1)

    def w_copy(k):
        return remote(wb.at[k], wb.at[k], snd_w.at[k], rec_w.at[k], c, r + 1)

    def each_row(first, fn):
        lax.fori_loop(first, K, lambda j, _: (fn(j), 0)[1], 0)

    def o_top():
        return remote(rst, trail_out.at[0:NB, :], snd_o.at[0], rec_o.at[0], c, r - 1)

    def o_low():
        return remote(ss.at[0:NB, :], trail_out.at[NB:2 * NB, :], snd_o.at[1], rec_o.at[1], c, r - 1)

    def o_row(s):
        return remote(rw.at[c + 4 * s, 0:NB, :], panel_out.at[s, NB:2 * NB, :], snd_o.at[2 + s], rec_o.at[2 + s], c, r - 1)

    z_send(0)

    @pl.when(is0)
    def _():
        @pl.when(p == 0)
        def _():
            got_a(0, 0)
            p_copy(0, 0, 0, px).start()
            p_copy(0, 0, 1, py).start()

        @pl.when(p != 0)
        def _():
            got_a(0, 0)

        @pl.when(p == 1)
        def _():
            p_copy(0, 0, 4, py).start()

        z_send(1)
        other_sends()

        def step(k, _):
            @pl.when(k > 0)
            def _():
                stage3(k, k)
                each_row(k - 1, lambda j: l_copy(k - 1, j).start())

            def left(m, _):
                rhs = col[m, rows_at(k), :]

                def upd(block, count):
                    sl = rows_at(block, count)
                    col[k, sl, :] = col[k, sl, :] - dot_nt(col[m, sl, :], rhs)

                over_rows(k, K, upd)
                return 0

            lax.fori_loop(0, k, left, 0)
            z[...] = col[k, rows_at(k), :]

            def at(b, when, fn):
                if b == when[0]:
                    @pl.when(when[1])
                    def _():
                        fn()

            def hook(b):
                at(b, (0, k == 0), lambda: stage1(0, 1))
                at(b, (1, k == 0), lambda: stage1(1, 1))
                at(b, (3, k == 0), lambda: stage2(0, 1))
                at(b, (5, k == 0), lambda: stage2(1, 1))
                at(b, (2, (k > 0) & (k < K - 1)), lambda: stage2(k + 1, k + 1))
                at(b, (6, k < K - 2), lambda: stage1(k + 2, k + 2))

            factor(z, lo, wb.at[k], hook)

            @pl.when(k == 0)
            def _():
                stage3(0, 1)

                @pl.when(p == 0)
                def _():
                    p_copy(0, 0, 0, px).wait_send()
                    p_copy(0, 0, 1, py).wait_send()

                @pl.when(p == 1)
                def _():
                    p_copy(0, 0, 4, py).wait_send()

            col[k, rows_at(k), :] = lo[...]
            w_copy(k).start()

            def solve(block, count):
                sl = rows_at(block, count)
                col[k, sl, :] = dot_nt(col[k, sl, :], wb[k])

            over_rows(k + 1, K, solve)
            return 0

        lax.fori_loop(0, K, step, 0)
        l_copy(K - 1, K - 1).start()

    @pl.when(is1)
    def _():
        z_send(1)
        other_sends()
        for i in (0, 1):
            pltpu.make_async_copy(ss.at[rows_at(i), :], ss.at[rows_at(i), :], rec_s.at[i]).wait()

        def step(k, _):
            pltpu.make_async_copy(tt.at[k], tt.at[k], rec_t.at[k]).wait()
            for i in (0, 1):
                pltpu.make_async_copy(rw.at[k, rows_at(i), :], rw.at[k, rows_at(i), :], rec_r.at[k, i]).wait()

            def left(m, _):
                got_a(m, k)
                lkm = col[m, rows_at(k), :]
                tt[k] = tt[k] - dot_nn(lkm, tt[m])
                rw[k] = rw[k] - dot_nt(rw[m], lkm)
                return 0

            lax.fori_loop(0, k, left, 0)

            @pl.when(k == r)
            def _():
                trail_out[0:NB, :] = tt[k]

            @pl.when(k == r - 1)
            def _():
                rst[...] = tt[k]

            pltpu.make_async_copy(wb.at[k], wb.at[k], rec_w.at[k]).wait()
            tt[k] = dot_nn(wb[k], tt[k])
            rw[k] = dot_nt(rw[k], wb[k])
            ss[...] = ss[...] - dot_nn(rw[k], tt[k])
            return 0

        lax.fori_loop(0, K, step, 0)
        o_low().start()
        o_row(0).start()
        o_row(1).start()
        o_top().start()
        trail_out[NB:2 * NB, :] = ss[NB:2 * NB, :]
        for s in (0, 1):
            panel_out[s, NB:2 * NB, :] = rw[c + 4 * s, NB:2 * NB, :]

        def diag_arrived(k, _):
            got_a(k, k)
            return 0

        lax.fori_loop(0, K, diag_arrived, 0)

    for s in (0, 1):
        k = c + 4 * s

        @pl.when(r >= k)
        def _(s=s, k=k):
            panel_out[s, 0:NB, :] = col[k, rows_at(r), :]

        @pl.when(r < k)
        def _(s=s):
            panel_out[s, 0:NB, :] = jnp.zeros((NB, NB), jnp.float32)

    z_done(0)
    z_done(1)
    other_done()

    @pl.when(is0)
    def _():
        def sent(k, _):
            w_copy(k).wait_send()
            each_row(k, lambda j: l_copy(k, j).wait_send())
            return 0

        lax.fori_loop(0, K, sent, 0)
        for ref, i in ((trail_out.at[0:NB, :], 0), (trail_out.at[NB:2 * NB, :], 1), (panel_out.at[0, NB:2 * NB, :], 2), (panel_out.at[1, NB:2 * NB, :], 3)):
            pltpu.make_async_copy(ref, ref, rec_o.at[i]).wait()

    @pl.when(is1)
    def _():
        o_low().wait_send()
        o_row(0).wait_send()
        o_row(1).wait_send()
        o_top().wait_send()


def solution(mesh):
    vmem = pl.BlockSpec(memory_space=pltpu.VMEM)
    f32 = jnp.float32
    dma = pltpu.SemaphoreType.DMA
    call = pl.pallas_call(
        chip_kernel,
        out_shape=[jax.ShapeDtypeStruct((2, 512, NB), f32), jax.ShapeDtypeStruct((512, 512), f32)],
        in_specs=[vmem, vmem],
        out_specs=[vmem, vmem],
        scratch_shapes=[
            pltpu.VMEM((K, K * NB, NB), f32),
            pltpu.VMEM((K, NB, NB), f32),
            pltpu.VMEM((K, 2 * NB, NB), f32),
            pltpu.VMEM((K, NB, 512), f32),
            pltpu.VMEM((512, 512), f32),
            pltpu.VMEM((NB, 512), f32),
            pltpu.VMEM((NB, NB), f32),
            pltpu.VMEM((NB, NB), f32),
            dma((K, K)), dma((K,)), dma((K,)), dma((K, 2)), dma((2,)), dma((4,)),
            dma((2, 4)), dma((K, 6)), dma((K, K)), dma((K,)), dma((4,)), dma((2, 4)), dma, dma((4,)),
        ],
        compiler_params=pltpu.CompilerParams(vmem_limit_bytes=60 * 1024 * 1024, has_side_effects=True),
    )

    def local_part(panel_tile, trail_tile):
        p, t = call(panel_tile.transpose(1, 0, 2), trail_tile)
        return p.transpose(1, 0, 2), t

    sp, st = P("pr", "pc", None), P("pr", "pc")
    return jax.shard_map(local_part, mesh=mesh, in_specs=(sp, st), out_specs=(sp, st), check_vma=False)
```

```python
import functools

import jax
import jax.numpy as jnp
from jax import lax
from jax.experimental import pallas as pl
from jax.experimental.pallas import tpu as pltpu
from jax.sharding import PartitionSpec as P

HI = lax.Precision.HIGHEST
NB = 256
B = 32
T = B // 8


def bc(v, s):
    return jnp.broadcast_to(v[s:s+1, :], (8, 128))

def factor(z, lout, wout, hook):
    sub = lax.broadcasted_iota(jnp.int32, (8,128), 0)
    lane = lax.broadcasted_iota(jnp.int32, (8,128), 1)
    for b in range(NB//B):
        r0 = b*B; v0 = r0//128; d0 = r0-128*v0
        hook(b)
        xa = [[z[r0+8*t:r0+8*t+8, 128*v:128*v+128] for v in range(v0,2)] for t in range(T)]
        cols = [[None]*T for _ in range(B)]
        for j in range(B):
            for t in range(j//8, T):
                cols[j][t] = jnp.broadcast_to(xa[t][0][:, d0+j:d0+j+1], (8,128))
        xs = []
        for t in range(T):
            row = list(xa[t])
            for v in range(v0):
                row.append(z[r0+8*t:r0+8*t+8, 128*v:128*v+128])
            e = jnp.where(lane < d0, xa[t][0], jnp.where(lane - d0 == sub + 8*t, 1.0, 0.0))
            row.append(e)
            xs.append(row)
        nv = len(xs[0])
        sv = [jnp.zeros((8,128), jnp.float32) for _ in range(T)]
        piv = bc(cols[0][0], 0)
        for p in range(B):
            tp, sp = divmod(p, 8)
            s = lax.rsqrt(piv)
            m = None
            if p < B-1:
                t1, s1 = divmod(p+1, 8)
                m = bc(cols[p][t1], s1)*s
                piv = bc(cols[p+1][t1], s1) - m*m
            l = [None]*T
            for t in range(tp, T):
                l[t] = cols[p][t]*s
            for j in range(p+1, B):
                mj = m if j == p+1 else bc(l[j//8], j%8)
                for t in range(j//8, T):
                    cols[j][t] = cols[j][t] - l[t]*mj
            lm = jnp.where(sub > sp, l[tp], 0.0)
            sv[tp] = jnp.where(sub == sp, s, sv[tp])
            for v in range(nv):
                u = bc(xs[tp][v], sp)*s
                if sp < 7:
                    xs[tp][v] = xs[tp][v] - lm*u
                for t in range(tp+1, T):
                    xs[t][v] = xs[t][v] - l[t]*u
        for t in range(T):
            for v in range(nv):
                xs[t][v] = xs[t][v]*sv[t]
        na = 2 - v0
        urow, rrow, wrow = [], [], []
        for t in range(T):
            a = list(xs[t][:na]); e = list(xs[t][na:])
            a0 = jnp.where(lane - d0 >= sub + 8*t, a[0], 0.0)
            ua = [jnp.zeros((8,128), jnp.float32)]*v0 + [a0] + a[1:]
            e[v0] = jnp.where(lane < d0 + B, e[v0], 0.0)
            wr = e + [jnp.zeros((8,128), jnp.float32)]*(1-v0)
            mid = jnp.where(lane < d0 + B, e[v0], a[0])
            rr = e[:v0] + [mid] + a[1:]
            urow.append(jnp.concatenate(ua, axis=1)); wrow.append(jnp.concatenate(wr, axis=1)); rrow.append(jnp.concatenate(rr, axis=1))
        U = jnp.concatenate(urow, axis=0); W = jnp.concatenate(wrow, axis=0); R = jnp.concatenate(rrow, axis=0)
        wout[r0:r0+B, :] = W
        LT = U.T
        lout[:, r0:r0+B] = LT
        lane2 = lax.broadcasted_iota(jnp.int32, (1, NB), 1)
        inb = (lane2 >= r0) & (lane2 < r0+B)
        def upd(lo, hi):
            if lo >= hi: return
            old = z[lo:hi, :]
            old = jnp.where(inb, 0.0, old)
            z[lo:hi, :] = old - lax.dot_general(LT[lo:hi], R, (((1,),(0,)),((),())), precision=HI, preferred_element_type=jnp.float32)
        upd(r0+B, min(r0+2*B, NB))
        upd(r0+2*B, NB)

MESH = pl.DeviceIdType.MESH
K = 8


def dot_nt(a, b):
    return lax.dot_general(a, b, (((1,), (1,)), ((), ())), precision=HI, preferred_element_type=jnp.float32)


def dot_nn(a, b):
    return lax.dot_general(a, b, (((1,), (0,)), ((), ())), precision=HI, preferred_element_type=jnp.float32)


def rows_at(block, count=1):
    return pl.ds(pl.multiple_of(block * NB, NB), count * NB)


def over_rows(first, stop, fn):
    total = stop - first

    def step(i, _):
        fn(first + 2 * i, 2)
        return 0

    lax.fori_loop(0, total // 2, step, 0)

    @pl.when(total % 2 == 1)
    def _():
        fn(stop - 1, 1)


def chip_kernel(panel, trail, panel_out, trail_out, ain, col, wb, rw, tt, ss, rst, z, lo,
                rec_a, rec_w, rec_t, rec_r, rec_s, rec_o, snd_z, snd_p, snd_l, snd_w, snd_t, snd_r, snd_s, snd_o, rec_b, snd_d):
    c = lax.axis_index("pc")
    r = lax.axis_index("pr")
    core = r % 2
    p = r // 2
    px = 2 * (p // 2) + (1 - p % 2)
    py = 2 * (1 - p // 2) + p % 2
    pd = 3 - p
    is0 = core == 0
    is1 = core == 1

    def remote(src, dst, send, recv, c2, r2):
        return pltpu.make_async_remote_copy(src_ref=src, dst_ref=dst, send_sem=send, recv_sem=recv, device_id=(c2, r2), device_id_type=MESH)

    def z_copy(s, i):
        k = c + 4 * s
        return remote(panel.at[s, 0:NB, :], ain.at[k, rows_at(r), :], snd_z.at[s, i], rec_b.at[k, r], (c + i) % 4, 2 * p + 1)

    def z_home(s):
        k = c + 4 * s
        return pltpu.make_async_copy(panel.at[s, 0:NB, :], ain.at[k, rows_at(r), :], rec_b.at[k, r])

    def z_send(s):
        @pl.when(r >= c + 4 * s)
        def _():
            for i in (1, 3, 2):
                z_copy(s, i).start()

        @pl.when((r >= c + 4 * s) & is1)
        def _():
            z_home(s).start()

        @pl.when((r >= c + 4 * s) & is0)
        def _():
            z_copy(s, 0).start()

    def z_done(s):
        @pl.when((r >= c + 4 * s) & is0)
        def _():
            z_copy(s, 0).wait_send()

        @pl.when(r >= c + 4 * s)
        def _():
            for i in (1, 2, 3):
                z_copy(s, i).wait_send()

    def t_copy(i):
        q = (p + i) % 4
        return remote(trail.at[0:NB, :], tt.at[r], snd_t.at[i], rec_t.at[r], c, 2 * q + 1)

    def r_copy(s, i):
        k = c + 4 * s
        return remote(panel.at[s, NB:2 * NB, :], rw.at[k, rows_at(core), :], snd_r.at[s, i], rec_r.at[k, core], (c + i) % 4, 2 * p + 1)

    def s_copy():
        return remote(trail.at[NB:2 * NB, :], ss.at[rows_at(core), :], snd_s, rec_s.at[core], c, r + 1)

    def other_sends():
        for i in (1, 2, 3):
            t_copy(i).start()
        for s in (0, 1):
            for i in (1, 3, 2):
                r_copy(s, i).start()

        @pl.when(is0)
        def _():
            t_copy(0).start()
            r_copy(0, 0).start()
            r_copy(1, 0).start()
            s_copy().start()

        @pl.when(is1)
        def _():
            pltpu.make_async_copy(trail.at[0:NB, :], tt.at[r], rec_t.at[r]).start()
            for s in (0, 1):
                pltpu.make_async_copy(panel.at[s, NB:2 * NB, :], rw.at[c + 4 * s, rows_at(core), :], rec_r.at[c + 4 * s, core]).start()
            pltpu.make_async_copy(trail.at[NB:2 * NB, :], ss.at[rows_at(core), :], rec_s.at[core]).start()

    def other_done():
        for i in (1, 2, 3):
            t_copy(i).wait_send()
            for s in (0, 1):
                r_copy(s, i).wait_send()

        @pl.when(is0)
        def _():
            t_copy(0).wait_send()
            r_copy(0, 0).wait_send()
            r_copy(1, 0).wait_send()
            s_copy().wait_send()

    def blk(k, j):
        return col.at[k, rows_at(j), :]

    def got_l(k, j):
        pltpu.make_async_copy(blk(k, j), blk(k, j), rec_a.at[k, j]).wait()

    def ablk(k, j):
        return ain.at[k, rows_at(j), :]

    def got_a(k, j):
        pltpu.make_async_copy(ablk(k, j), ablk(k, j), rec_b.at[k, j]).wait()

    def p_copy(k, j, n, q):
        return remote(ablk(k, j), ablk(k, j), snd_p.at[k, n], rec_b.at[k, j], c, 2 * q + (1 if n in (0, 2) else 0))

    def d_copy(k, j, n):
        return remote(ablk(k, j), ablk(k, j), snd_d.at[k, n], rec_b.at[k, j], c, r - 1)

    even, odd = 2 * p, 2 * p + 1
    stage1_sends = ((even, (0, px), (1, py), 0), (odd, (2, py), (3, px), 1))
    stage2_sends = ((2 * px, (4, py), None, 2), (2 * py + 1, (5, px), None, 3))

    def relay(k, lowest, sends, act, first):
        for j, one, two, n in sends:
            @pl.when((j >= lowest) & (j >= k))
            def _(j=j, one=one, two=two, n=n):
                if first:
                    got_a(k, j)
                act(d_copy(k, j, n))
                act(p_copy(k, j, *one))
                if two is not None:
                    act(p_copy(k, j, *two))

    def start(copy):
        copy.start()

    def finish(copy):
        copy.wait_send()

    def stage1(k):
        relay(k, 1, stage1_sends, start, True)

    def stage2(k):
        relay(k, 1, stage2_sends, start, True)

    def first_block(act, first):
        for here, sends in ((p == 0, stage1_sends[0]), (p == 1, stage2_sends[0])):
            @pl.when(here)
            def _(sends=sends):
                j, one, two, n = sends
                if first:
                    got_a(0, j)
                act(p_copy(0, j, *one))
                if two is not None:
                    act(p_copy(0, j, *two))
                act(d_copy(0, j, n))

    def got_rows(k, first):
        lax.fori_loop(first, K, lambda j, _: (got_a(k, j), 0)[1], 0)

    def l_copy(k, j):
        return remote(blk(k, j), blk(k, j), snd_l.at[k, j], rec_a.at[k, j], c, r + 1)

    def w_copy(k):
        return remote(wb.at[k], wb.at[k], snd_w.at[k], rec_w.at[k], c, r + 1)

    def each_row(first, fn):
        lax.fori_loop(first, K, lambda j, _: (fn(j), 0)[1], 0)

    def o_top():
        return remote(rst, trail_out.at[0:NB, :], snd_o.at[0], rec_o.at[0], c, r - 1)

    def o_low():
        return remote(ss.at[0:NB, :], trail_out.at[NB:2 * NB, :], snd_o.at[1], rec_o.at[1], c, r - 1)

    def o_row(s):
        return remote(rw.at[c + 4 * s, 0:NB, :], panel_out.at[s, NB:2 * NB, :], snd_o.at[2 + s], rec_o.at[2 + s], c, r - 1)

    z_send(0)
    z_send(1)

    @pl.when(is0)
    def _():
        other_sends()
        got_a(0, 0)

        def step(k, _):
            q = jnp.maximum(k - 1, 0)
            left = K - 1 - k
            each = jnp.maximum(left, 1)

            @pl.when(k > 0)
            def _():
                col[q, rows_at(k), :] = dot_nt(ain[q, rows_at(k), :], wb[q])
                w_copy(q).start()
                l_kq = col[q, rows_at(k), :]
                z[...] = ain[k, rows_at(k), :] - dot_nt(l_kq, l_kq)
                l_copy(q, k).start()

            @pl.when(k == 0)
            def _():
                z[...] = ain[0, 0:NB, :]

            def solve_task(i):
                j = jnp.where((i < left) & (k > 0), k + 1 + i, K)
                src = jnp.where((i < left) & (k > 0), k + 1 + i, 0)
                col[q, rows_at(j), :] = dot_nt(ain[q, rows_at(src), :], wb[q])

            def update_task(t):
                u = t - left
                m = jnp.where(u < 0, q, u // each)
                i = jnp.where(u < 0, t, u % each)
                live = (left > 0) & (m < k)
                dst_col = jnp.where(live, jnp.where(u < 0, k, k + 1), 0)
                dst_row = jnp.where(live, k + 1 + i, K)
                m = jnp.where(live, m, 0)
                j = jnp.where(live, k + 1 + i, 0)
                y = jnp.where(live, dst_col, 0)
                ain[dst_col, rows_at(dst_row), :] = ain[dst_col, rows_at(dst_row), :] - dot_nt(col[m, rows_at(j), :], col[m, rows_at(y), :])

            def at(b, when, fn):
                if b == when[0]:
                    @pl.when(when[1])
                    def _():
                        fn()

            def hook(b):
                at(b, (0, k == 1), lambda: got_rows(0, 2))
                at(b, (0, k == 1), lambda: got_rows(1, 2))
                at(b, (2, (k > 0) & (k < K - 1)), lambda: got_rows(k + 1, k + 1))
                if b < 2:
                    for i in range(3):
                        solve_task(3 * b + i)
                else:
                    first = (0, 3, 6, 9, 12, 14, 16)
                    for t in range(first[b - 2], first[b - 1]):
                        update_task(t)

            factor(z, lo, wb.at[k], hook)
            col[k, rows_at(k), :] = lo[...]

            @pl.when(k == 0)
            def _():
                got_a(0, 1)
                got_a(1, 1)

            @pl.when(k > 0)
            def _():
                lax.fori_loop(k + 1, K, lambda j, _: (l_copy(q, j).start(), 0)[1], 0)

            l_copy(k, k).start()
            return 0

        lax.fori_loop(0, K, step, 0)
        w_copy(K - 1).start()

    @pl.when(is1)
    def _():
        other_sends()
        first_block(start, True)
        stage1(0)
        stage1(1)
        stage2(0)
        for n in range(2, 8):
            stage1(n)
            stage2(n - 1)
        stage2(7)
        for i in (0, 1):
            pltpu.make_async_copy(ss.at[rows_at(i), :], ss.at[rows_at(i), :], rec_s.at[i]).wait()

        def step(k, _):
            pltpu.make_async_copy(tt.at[k], tt.at[k], rec_t.at[k]).wait()
            for i in (0, 1):
                pltpu.make_async_copy(rw.at[k, rows_at(i), :], rw.at[k, rows_at(i), :], rec_r.at[k, i]).wait()

            def left(m, _):
                got_l(m, k)
                lkm = col[m, rows_at(k), :]
                tt[k] = tt[k] - dot_nn(lkm, tt[m])
                rw[k] = rw[k] - dot_nt(rw[m], lkm)
                return 0

            lax.fori_loop(0, k, left, 0)

            @pl.when(k == r)
            def _():
                trail_out[0:NB, :] = tt[k]

            @pl.when(k == r - 1)
            def _():
                rst[...] = tt[k]

            pltpu.make_async_copy(wb.at[k], wb.at[k], rec_w.at[k]).wait()
            tt[k] = dot_nn(wb[k], tt[k])
            rw[k] = dot_nt(rw[k], wb[k])
            ss[...] = ss[...] - dot_nn(rw[k], tt[k])
            return 0

        lax.fori_loop(0, K, step, 0)
        o_low().start()
        o_row(0).start()
        o_row(1).start()
        o_top().start()
        trail_out[NB:2 * NB, :] = ss[NB:2 * NB, :]
        for s in (0, 1):
            panel_out[s, NB:2 * NB, :] = rw[c + 4 * s, NB:2 * NB, :]

        def diag_arrived(k, _):
            got_l(k, k)
            return 0

        lax.fori_loop(0, K, diag_arrived, 0)

    for s in (0, 1):
        k = c + 4 * s

        @pl.when(r >= k)
        def _(s=s, k=k):
            panel_out[s, 0:NB, :] = col[k, rows_at(r), :]

        @pl.when(r < k)
        def _(s=s):
            panel_out[s, 0:NB, :] = jnp.zeros((NB, NB), jnp.float32)

    z_done(0)
    z_done(1)
    other_done()

    @pl.when(is0)
    def _():
        def sent(k, _):
            w_copy(k).wait_send()
            each_row(k, lambda j: l_copy(k, j).wait_send())
            return 0

        lax.fori_loop(0, K, sent, 0)
        for ref, i in ((trail_out.at[0:NB, :], 0), (trail_out.at[NB:2 * NB, :], 1), (panel_out.at[0, NB:2 * NB, :], 2), (panel_out.at[1, NB:2 * NB, :], 3)):
            pltpu.make_async_copy(ref, ref, rec_o.at[i]).wait()

    @pl.when(is1)
    def _():
        first_block(finish, False)

        def passed(k, _):
            relay(k, 1, stage1_sends, finish, False)
            relay(k, 1, stage2_sends, finish, False)
            return 0

        lax.fori_loop(0, K, passed, 0)
        o_low().wait_send()
        o_row(0).wait_send()
        o_row(1).wait_send()
        o_top().wait_send()


def solution(mesh):
    vmem = pl.BlockSpec(memory_space=pltpu.VMEM)
    f32 = jnp.float32
    dma = pltpu.SemaphoreType.DMA
    call = pl.pallas_call(
        chip_kernel,
        out_shape=[jax.ShapeDtypeStruct((2, 512, NB), f32), jax.ShapeDtypeStruct((512, 512), f32)],
        in_specs=[vmem, vmem],
        out_specs=[vmem, vmem],
        scratch_shapes=[
            pltpu.VMEM((K, (K + 1) * NB, NB), f32),
            pltpu.VMEM((K, (K + 1) * NB, NB), f32),
            pltpu.VMEM((K, NB, NB), f32),
            pltpu.VMEM((K, 2 * NB, NB), f32),
            pltpu.VMEM((K, NB, 512), f32),
            pltpu.VMEM((512, 512), f32),
            pltpu.VMEM((NB, 512), f32),
            pltpu.VMEM((NB, NB), f32),
            pltpu.VMEM((NB, NB), f32),
            dma((K, K)), dma((K,)), dma((K,)), dma((K, 2)), dma((2,)), dma((4,)),
            dma((2, 4)), dma((K, 6)), dma((K, K)), dma((K,)), dma((4,)), dma((2, 4)), dma, dma((4,)), dma((K, K)), dma((K, 4)),
        ],
        compiler_params=pltpu.CompilerParams(vmem_limit_bytes=60 * 1024 * 1024, has_side_effects=True),
    )

    def local_part(panel_tile, trail_tile):
        p, t = call(panel_tile.transpose(1, 0, 2), trail_tile)
        return p.transpose(1, 0, 2), t

    sp, st = P("pr", "pc", None), P("pr", "pc")
    return jax.shard_map(local_part, mesh=mesh, in_specs=(sp, st), out_specs=(sp, st), check_vma=False)
```
